32 devices in a mesh: arm: 2 (over y), snp: 16 (over z, x, core).
Axes of the slice: x: 2, y: 2, z: 4, core: 2. Of those that a mesh axis runs over, the one named last changes fastest.
Arguments:
- genotypes: int32 [4096, 1024], P(('arm', 'snp')), parts along dimension 0, may hold values from -2147483648 to 2147483647, as said below
- positions: int32 [4096], P(('arm', 'snp')), parts along dimension 0, may hold values from 2001303 to 5334144, as said below
Outputs:
- linkage: float32 [4096, 1664], P(('arm', 'snp')), parts along dimension 0
The draws below stay inside these ranges and needn't reach their ends.
There are 2 independent parts, one for each index of `arm`. The reference program is written for one: setup_inputs(seed, part) draws one part's arguments, and reference() takes and returns one part's arrays. A program takes and returns all parts, laid end to end along the dimension named above; each array names one. Nothing has to cross between parts.
Inputs may be any that keep to these rules, and one draw needn't show every extreme that they name: `genotypes`: each word holds 16 two-bit codes: the call of sample s sits in bits 2 * (s // 1024) and 2 * (s // 1024) + 1 of word s mod 1024; codes 0, 1, 2 count alternate alleles and code 3 marks a missing call. `positions`: strictly increasing; consecutive SNPs lie 1303 or more base pairs apart.
All inputs are finite; a program needn't handle non-finite values.
Results may differ from the reference program's by a relative error of at most 0.0031.
Values may be sent and summed in bfloat16 or wider, within the bound.
A program may use at most 128 MiB of HBM per device.

```python
import jax
import jax.numpy as jnp
from jax import lax

SNP_DEV = 128
SAMPLES = 16384
REACH = 6
BAND_BP = 1000000
WORDS = 1024
SNPS = 2048
GAP_MIN = 1303
N_SNP = 16


def draw_genotypes(key, part):
    keys = jax.random.split(jax.random.fold_in(key, 11), 8)
    thresh = jax.random.randint(keys[0], (SNPS, 1), 50, 950)
    offset = jax.random.randint(keys[1], (), 0, 24)
    block_id = (jnp.arange(SNPS, dtype=jnp.int32) + offset) // 24
    nblocks = SNPS // 24 + 2
    dosage = jnp.zeros((SNPS, SAMPLES), jnp.int32)
    for strand in range(2):
        shared = jax.random.randint(keys[2 + strand], (nblocks, SAMPLES), 0, 1000)
        fresh = jax.random.randint(keys[4 + strand], (SNPS, SAMPLES), 0, 4000)
        latent = jnp.where(fresh < 1000, fresh, shared[block_id])
        dosage = dosage + (latent < thresh).astype(jnp.int32)
    missing = jax.random.randint(keys[6], (SNPS, SAMPLES), 0, 25) == 0
    codes = jnp.where(missing, 3, dosage).astype(jnp.int32)
    grouped = codes.reshape(SNPS, 16, WORDS)
    packed = jnp.zeros((SNPS, WORDS), jnp.int32)
    for lane in range(16):
        packed = packed | jnp.left_shift(grouped[:, lane, :], 2 * lane)
    return packed


def draw_positions(key, part):
    keys = jax.random.split(jax.random.fold_in(key, 23), 1)
    gaps = jax.random.randint(keys[0], (SNPS,), GAP_MIN, GAP_MIN + GAP_MIN // 4 + 1).astype(jnp.int32)
    top_value = 2 * BAND_BP + SNPS * (GAP_MIN + GAP_MIN // 4)
    running = jnp.cumsum(gaps).astype(jnp.int32)
    return (top_value - (running[-1] - running)).astype(jnp.int32)


def setup_inputs(seed: int = 0, part: int = 0) -> dict:
    seeds = jax.random.split(jax.random.key(seed), 3)
    part_keys = jax.random.split(jax.random.fold_in(seeds[2], part), 3)
    genotypes = draw_genotypes(jax.random.fold_in(jax.random.fold_in(seeds[2], part), 71), part)
    positions = draw_positions(jax.random.fold_in(jax.random.fold_in(seeds[2], part), 71), part)
    return dict(genotypes=genotypes, positions=positions)


def standardize(packed):
    shifts = 2 * jnp.arange(16, dtype=jnp.int32)
    codes = jnp.right_shift(packed[:, None, :], shifts[None, :, None]) & 3
    called = codes != 3
    observed = called.astype(jnp.float32)
    dosage = jnp.where(called, codes, 0).astype(jnp.float32)
    tally = lax.optimization_barrier(jnp.sum(observed, axis=(1, 2)))
    allele = (lax.optimization_barrier(jnp.sum(dosage, axis=(1, 2))) + 1.0) / (2.0 * tally + 2.0)
    spread = lax.rsqrt(2.0 * allele * (1.0 - allele))
    scores = observed * (dosage - 2.0 * allele[:, None, None]) * spread[:, None, None]
    return scores.astype(jnp.bfloat16)

def reference(genotypes, positions):
    blocks = genotypes.reshape(N_SNP, SNP_DEV, WORDS)
    scored = lax.map(standardize, blocks)
    scored = lax.optimization_barrier(scored)
    flat = scored.astype(jnp.float32).reshape(SNPS, SAMPLES)
    margin = REACH * SNP_DEV
    padded = jnp.pad(flat, ((margin, margin), (0, 0)))
    pos_pad = jnp.pad(positions, (margin, margin))
    inside = jnp.pad(jnp.ones((SNPS,), jnp.int32), (margin, margin))
    span = (2 * REACH + 1) * SNP_DEV

    def window(index):
        first = (index * SNP_DEV).astype(jnp.int32)
        rows = lax.dynamic_slice_in_dim(flat, first, SNP_DEV, 0)
        columns = lax.dynamic_slice_in_dim(padded, first, span, 0)
        product = jnp.dot(rows, columns.T, precision=lax.Precision.HIGHEST, preferred_element_type=jnp.float32) / SAMPLES
        row_pos = lax.dynamic_slice_in_dim(positions, first, SNP_DEV, 0)
        col_pos = lax.dynamic_slice_in_dim(pos_pad, first, span, 0)
        col_in = lax.dynamic_slice_in_dim(inside, first, span, 0)
        in_band = (jnp.abs(row_pos[:, None] - col_pos[None, :]) <= BAND_BP) & (col_in[None, :] == 1)
        return jnp.where(in_band, product, jnp.zeros_like(product))
    result = lax.map(window, jnp.arange(N_SNP, dtype=jnp.int32))
    return result.reshape(SNPS, span)
```

```python
import functools

import jax
import jax.numpy as jnp
from jax import lax
from jax.experimental import pallas as pl
from jax.experimental.pallas import tpu as pltpu
from jax.sharding import PartitionSpec as P

REACH = 6
BAND_BP = 1000000
CODES = 16
GROUP = 4
SPLIT = 4096
MESH = pl.DeviceIdType.MESH


def kernel(
    devices, geno, pos, out, words, stats, scores, accs, parts, gathered, mirror, came,
    w0s, w0r, w1s, w1r, w2s, w2r, s0s, s0r, s1s, s1r, s2s, s2r, ps, pr, ms, mr,
):
    rows, width = geno.shape
    quarter = width // GROUP
    groups = devices // GROUP
    samples = CODES * width
    me = lax.axis_index("snp")
    g, q = me // GROUP, me % GROUP
    base = me - q
    mates = [q + 1 - 2 * lax.rem(q, 2), lax.rem(q + 2, GROUP), None]
    mates[2] = mates[1] + 1 - 2 * lax.rem(mates[1], 2)

    def remote(src, dst, ss, rs, target):
        return pltpu.make_async_remote_copy(
            src_ref=src, dst_ref=dst, send_sem=ss, recv_sem=rs,
            device_id={"snp": target}, device_id_type=MESH,
        )

    barrier = pltpu.get_barrier_semaphore()
    for mate in mates:
        pl.semaphore_signal(barrier, inc=1, device_id={"snp": base + mate}, device_id_type=MESH)
    for dg in (-2, -1, 1, 2):
        @pl.when((g + dg >= 0) & (g + dg < groups))
        def _():
            for m in range(GROUP):
                pl.semaphore_signal(
                    barrier, inc=1, device_id={"snp": base + dg * GROUP + m}, device_id_type=MESH
                )

    low = 0x55555555
    raw = geno[...]
    up = jnp.right_shift(raw, 1)
    miss = raw & up & low
    ones = raw & low & ~miss
    twos = up & low & ~miss

    def count(x):
        x = (x & 0x33333333) + (jnp.right_shift(x, 2) & 0x33333333)
        x = (x & 0x0F0F0F0F) + (jnp.right_shift(x, 4) & 0x0F0F0F0F)
        x = x + jnp.right_shift(x, 8)
        x = (x + jnp.right_shift(x, 16)) & 0x3F
        return jnp.sum(x.astype(jnp.float32), axis=1, keepdims=True)

    tally = samples - count(miss)
    allele = (count(ones) + 2.0 * count(twos) + 1.0) / (2.0 * tally + 2.0)
    spread = lax.rsqrt(2.0 * allele * (1.0 - allele))
    lane = lax.broadcasted_iota(jnp.int32, (rows, 128), 1)
    pair_t = jnp.where(lane < 2, 2.0 * allele, spread).T
    where_row = pos[...]
    hi = where_row // SPLIT
    lo = where_row - hi * SPLIT
    stats[0, q, 0:4, :] = pair_t[0:4, :]
    stats[0, q, 4:6, :] = jnp.broadcast_to(hi.astype(jnp.float32), (2, rows))
    stats[0, q, 6:8, :] = jnp.broadcast_to(lo.astype(jnp.float32), (2, rows))
    own_cols = pl.ds(pl.multiple_of(q * quarter, quarter), quarter)
    words[0, q] = geno[:, own_cols]
    out[...] = jnp.zeros_like(out)

    near = jnp.minimum(g, 2) + jnp.minimum(groups - 1 - g, 2)
    pl.semaphore_wait(barrier, 3 + GROUP * near)

    def word_copy(i):
        mate = mates[i]
        cols = pl.ds(pl.multiple_of(mate * quarter, quarter), quarter)
        return remote(geno.at[:, cols], words.at[0, q], w0s.at[i], w0r.at[q], base + mate)

    def down_one(m, src):
        return remote(src, words.at[1, m], w1s.at[m], w1r.at[m], me - GROUP)

    def down_two(m, src):
        return remote(src, words.at[2, m], w2s.at[m], w2r.at[m], me - 2 * GROUP)

    def stat_mate(i):
        return remote(stats.at[0, q], stats.at[0, q], s0s.at[i], s0r.at[q], base + mates[i])

    def stat_one(m):
        return remote(stats.at[0, q], stats.at[1, q], s1s.at[m], s1r.at[q], base - GROUP + m)

    def stat_two(m):
        return remote(stats.at[0, q], stats.at[2, q], s2s.at[m], s2r.at[q], base - 2 * GROUP + m)

    has_one, has_two = g >= 1, g >= 2
    up_one, up_two = g + 1 < groups, g + 2 < groups

    for i in range(3):
        word_copy(i).start()
    for i in range(3):
        stat_mate(i).start()

    @pl.when(has_one)
    def _():
        for m in range(GROUP):
            stat_one(m).start()
        down_one(q, geno.at[:, own_cols]).start()

    @pl.when(has_two & (q < 2))
    def _():
        for m in range(GROUP):
            stat_two(m).start()
        down_two(q, geno.at[:, own_cols]).start()

    def wait_recv(ref, sem):
        remote(ref, ref, sem, sem, me).wait_recv()

    def decode(dg, m, slot, row0):
        st = jnp.concatenate([stats[dg, m]] * (rows // 8), axis=0).T
        mean, dev = st[:, 0:1], st[:, 2:3]
        packed = words[dg, m]

        def step(k, _):
            code = jnp.right_shift(packed, 2 * k) & 3
            z = (code.astype(jnp.float32) - mean) * dev
            z = jnp.where(code == 3, 0.0, z).astype(jnp.bfloat16)
            scores[slot, pl.ds(pl.multiple_of(row0, rows), rows),
                   pl.ds(pl.multiple_of(k * quarter, quarter), quarter)] = z
            return 0

        lax.fori_loop(0, CODES, step, 0, unroll=2)

    decode(0, q, q // 2, (q % 2) * rows)
    for mate in mates:
        wait_recv(words.at[0, mate], w0r.at[mate])

        @pl.when(has_one)
        def _():
            down_one(mate, words.at[0, mate]).start()

        @pl.when(has_two & (mate < 2))
        def _():
            down_two(mate, words.at[0, mate]).start()

        wait_recv(stats.at[0, mate], s0r.at[mate])
        decode(0, mate, mate // 2, (mate % 2) * rows)

    def part_copy(t, i):
        return remote(parts.at[t, mates[i]], gathered.at[t, q], ps.at[t, i], pr.at[t, q], base + mates[i])

    def product(t, slot, first):
        right = scores[slot]
        for half in range(first, 2):
            block = lax.dot_general(
                scores[half], right, (((1,), (1,)), ((), ())), preferred_element_type=jnp.float32
            )
            accs[t, 2 * half] = block[:rows]
            accs[t, 2 * half + 1] = block[rows:]
            parts[t, 2 * half] = block[:rows].astype(jnp.bfloat16)
            parts[t, 2 * half + 1] = block[rows:].astype(jnp.bfloat16)

    first_pair = q // 2
    steps = [(0, first_pair), (0, 1 - first_pair), (1, first_pair), (1, 1 - first_pair), (2, 0)]
    slots = [first_pair, 1 - first_pair, 2 + first_pair, 3 - first_pair, 4]

    own_pos = jnp.concatenate([stats[0, q]] * (rows // 8), axis=0).T
    own_at = own_pos[:, 4:5].astype(jnp.int32) * SPLIT + own_pos[:, 6:7].astype(jnp.int32)

    def mirror_copy(t, m2, offset):
        return remote(
            mirror.at[t, m2], came.at[offset - 1], ms.at[t, m2], mr.at[offset - 1], me + offset
        )

    def finish(n):
        dg, pair = steps[n]
        t = slots[n]
        total = accs[t, q]
        for mate in mates:
            wait_recv(gathered.at[t, mate], pr.at[t, mate])
            total = total + gathered[t, mate].astype(jnp.float32)
        total = total / samples
        for m2 in range(2):
            m = 2 * pair + m2
            offset = dg * GROUP + m - q
            st = stats[dg, m]
            their = st[4:5, :].astype(jnp.int32) * SPLIT + st[6:7, :].astype(jnp.int32)
            block = total[:, m2 * rows:(m2 + 1) * rows]
            block = jnp.where(jnp.abs(own_at - their) <= BAND_BP, block, 0.0)
            cols = pl.ds(pl.multiple_of((REACH + offset) * rows, rows), rows)
            if dg == 0:
                out[:, cols] = block
            else:
                @pl.when(offset <= REACH)
                def _():
                    out[:, cols] = block
                    mirror[t, m2] = block.astype(jnp.bfloat16)
                    mirror_copy(t, m2, offset).start()

    def run(n):
        dg, pair = steps[n]
        if dg == 0:
            slot = pair
        else:
            slot = n
            for m2 in range(2):
                m = 2 * pair + m2
                wait_recv(words.at[dg, m], (w1r if dg == 1 else w2r).at[m])
                wait_recv(stats.at[dg, m], (s1r if dg == 1 else s2r).at[m])
                decode(dg, m, slot, m2 * rows)
        product(slots[n], slot, 1 if dg == 2 else 0)
        for i in range(3):
            if dg == 2:
                @pl.when(mates[i] >= 2)
                def _():
                    part_copy(slots[n], i).start()
            else:
                part_copy(slots[n], i).start()

    run(0)
    run(1)

    @pl.when(up_one)
    def _():
        run(2)
        finish(0)
        finish(1)
        run(3)
        finish(2)

    @pl.when(jnp.logical_not(up_one))
    def _():
        finish(0)
        finish(1)

    @pl.when(up_two)
    def _():
        run(4)

    @pl.when(up_one)
    def _():
        finish(3)

    @pl.when(up_two & (q >= 2))
    def _():
        finish(4)

    for offset in range(1, REACH + 1):
        @pl.when((offset > q) & (me >= offset))
        def _():
            wait_recv(came.at[offset - 1], mr.at[offset - 1])
            out[:, (REACH - offset) * rows:(REACH - offset + 1) * rows] = (
                came[offset - 1].astype(jnp.float32).T
            )

    for i in range(3):
        word_copy(i).wait_send()
        stat_mate(i).wait_send()
        part_copy(slots[0], i).wait_send()
        part_copy(slots[1], i).wait_send()

    @pl.when(has_one)
    def _():
        for m in range(GROUP):
            stat_one(m).wait_send()
            down_one(m, words.at[0, m]).wait_send()

    @pl.when(has_two)
    def _():
        for m in range(2):
            down_two(m, words.at[0, m]).wait_send()

    @pl.when(has_two & (q < 2))
    def _():
        for m in range(GROUP):
            stat_two(m).wait_send()

    @pl.when(up_one)
    def _():
        for n in (2, 3):
            for i in range(3):
                part_copy(slots[n], i).wait_send()

    @pl.when(up_two)
    def _():
        for i in range(3):
            @pl.when(mates[i] >= 2)
            def _():
                part_copy(slots[4], i).wait_send()

    for n, there in ((2, up_one), (3, up_one), (4, up_two & (q >= 2))):
        dg, pair = steps[n]
        for m2 in range(2):
            offset = dg * GROUP + 2 * pair + m2 - q

            @pl.when(there & (offset <= REACH))
            def _():
                mirror_copy(slots[n], m2, offset).wait_send()


def per_device(devices, genotypes, positions):
    rows, width = genotypes.shape
    quarter = width // GROUP
    dma = pltpu.SemaphoreType.DMA
    vmem = pl.BlockSpec(memory_space=pltpu.VMEM)
    return pl.pallas_call(
        functools.partial(kernel, devices),
        out_shape=jax.ShapeDtypeStruct((rows, (2 * REACH + 1) * rows), jnp.float32),
        in_specs=[vmem, vmem],
        out_specs=vmem,
        scratch_shapes=[
            pltpu.VMEM((3, GROUP, rows, quarter), jnp.int32),
            pltpu.VMEM((3, GROUP, 8, rows), jnp.float32),
            pltpu.VMEM((5, 2 * rows, CODES * quarter), jnp.bfloat16),
            pltpu.VMEM((5, GROUP, rows, 2 * rows), jnp.float32),
            pltpu.VMEM((5, GROUP, rows, 2 * rows), jnp.bfloat16),
            pltpu.VMEM((5, GROUP, rows, 2 * rows), jnp.bfloat16),
            pltpu.VMEM((5, 2, rows, rows), jnp.bfloat16),
            pltpu.VMEM((REACH, rows, rows), jnp.bfloat16),
            dma((3,)), dma((GROUP,)),
            dma((GROUP,)), dma((GROUP,)),
            dma((GROUP,)), dma((GROUP,)),
            dma((3,)), dma((GROUP,)),
            dma((GROUP,)), dma((GROUP,)),
            dma((GROUP,)), dma((GROUP,)),
            dma((5, 3)), dma((5, GROUP)),
            dma((5, 2)), dma((REACH,)),
        ],
        compiler_params=pltpu.CompilerParams(
            collective_id=0, has_side_effects=True, vmem_limit_bytes=60000000
        ),
    )(genotypes, positions[None, :])


def solution(mesh):
    return jax.shard_map(
        functools.partial(per_device, mesh.shape["snp"]),
        mesh=mesh,
        in_specs=(P(("arm", "snp"), None), P(("arm", "snp"))),
        out_specs=P(("arm", "snp"), None),
        check_vma=False,
    )
```

```python
import functools

import jax
import jax.numpy as jnp
from jax import lax
from jax.experimental import pallas as pl
from jax.experimental.pallas import tpu as pltpu
from jax.sharding import PartitionSpec as P

REACH = 6
BAND_BP = 1000000
CODES = 16
GROUP = 4
SPLIT = 4096
MESH = pl.DeviceIdType.MESH


def kernel(
    devices, geno, pos, out, words, stats, scores, accs, parts, gathered, sums, mirror, came, spans,
    w0s, w0r, w1s, w1r, w2s, w2r, s0s, s0r, s1s, s1r, s2s, s2r, ps, pr, ms, mr,
):
    rows, width = geno.shape
    quarter = width // GROUP
    groups = devices // GROUP
    samples = CODES * width
    me = lax.axis_index("snp")
    g, q = me // GROUP, me % GROUP
    base = me - q
    mates = [q + 1 - 2 * lax.rem(q, 2), lax.rem(q + 2, GROUP), None]
    mates[2] = mates[1] + 1 - 2 * lax.rem(mates[1], 2)

    def remote(src, dst, ss, rs, target):
        return pltpu.make_async_remote_copy(
            src_ref=src, dst_ref=dst, send_sem=ss, recv_sem=rs,
            device_id={"snp": target}, device_id_type=MESH,
        )

    barrier = pltpu.get_barrier_semaphore()
    for mate in mates:
        pl.semaphore_signal(barrier, inc=1, device_id={"snp": base + mate}, device_id_type=MESH)
    for dg in (-2, -1, 1, 2):
        @pl.when((g + dg >= 0) & (g + dg < groups))
        def _():
            for m in range(GROUP):
                pl.semaphore_signal(
                    barrier, inc=1, device_id={"snp": base + dg * GROUP + m}, device_id_type=MESH
                )

    low = 0x55555555
    raw = geno[...]
    up = jnp.right_shift(raw, 1)
    miss = raw & up & low
    ones = raw & low & ~miss
    twos = up & low & ~miss

    def count(x):
        x = (x & 0x33333333) + (jnp.right_shift(x, 2) & 0x33333333)
        x = (x & 0x0F0F0F0F) + (jnp.right_shift(x, 4) & 0x0F0F0F0F)
        x = x + jnp.right_shift(x, 8)
        x = (x + jnp.right_shift(x, 16)) & 0x3F
        return jnp.sum(x.astype(jnp.float32), axis=1, keepdims=True)

    tally = samples - count(miss)
    allele = (count(ones) + 2.0 * count(twos) + 1.0) / (2.0 * tally + 2.0)
    spread = lax.rsqrt(2.0 * allele * (1.0 - allele))
    lane = lax.broadcasted_iota(jnp.int32, (rows, 128), 1)
    pair_t = jnp.where(lane < 2, 2.0 * allele, spread).T
    where_row = pos[...]
    hi = where_row // SPLIT
    lo = where_row - hi * SPLIT
    stats[0, q, 0:4, :] = pair_t[0:4, :]
    stats[0, q, 4:6, :] = jnp.broadcast_to(hi.astype(jnp.float32), (2, rows))
    stats[0, q, 6:8, :] = jnp.broadcast_to(lo.astype(jnp.float32), (2, rows))
    own_cols = pl.ds(pl.multiple_of(q * quarter, quarter), quarter)
    words[0, q] = geno[:, own_cols]
    out[...] = jnp.zeros_like(out)

    near = jnp.minimum(g, 2) + jnp.minimum(groups - 1 - g, 2)
    pl.semaphore_wait(barrier, 3 + GROUP * near)

    def word_copy(i):
        mate = mates[i]
        cols = pl.ds(pl.multiple_of(mate * quarter, quarter), quarter)
        return remote(geno.at[:, cols], words.at[0, q], w0s.at[i], w0r.at[q], base + mate)

    def down_one(m, src):
        return remote(src, words.at[1, m], w1s.at[m], w1r.at[m], me - GROUP)

    def up_words(m, src):
        return remote(src, words.at[2, m - 2], w2s.at[m - 2], w2r.at[m - 2], me + 2 * GROUP)

    def stat_mate(i):
        return remote(stats.at[0, q], stats.at[0, q], s0s.at[i], s0r.at[q], base + mates[i])

    def stat_one(m):
        return remote(stats.at[0, q], stats.at[1, q], s1s.at[m], s1r.at[q], base - GROUP + m)

    def stat_two(m):
        return remote(stats.at[0, q], stats.at[2, q - 2], s2s.at[m], s2r.at[q - 2], base + 2 * GROUP + m)

    has_one, has_two = g >= 1, g >= 2
    up_one, up_two = g + 1 < groups, g + 2 < groups

    for i in range(3):
        word_copy(i).start()
    for i in range(3):
        stat_mate(i).start()

    @pl.when(has_one)
    def _():
        for m in range(GROUP):
            stat_one(m).start()
        down_one(q, geno.at[:, own_cols]).start()

    @pl.when(up_two & (q >= 2))
    def _():
        for m in range(GROUP):
            stat_two(m).start()
        up_words(q, geno.at[:, own_cols]).start()

    def wait_recv(ref, sem):
        remote(ref, ref, sem, sem, me).wait_recv()

    def decode(dg, m, slot, row0):
        st = jnp.concatenate([stats[dg, m]] * (rows // 8), axis=0).T
        spans[0] = jnp.broadcast_to(st[:, 0:1], (rows, 128))
        spans[1] = jnp.broadcast_to(st[:, 2:3], (rows, 128))

        def step(r, _):
            some = pl.ds(pl.multiple_of(r * 16, 16), 16)
            there = pl.ds(pl.multiple_of(row0 + r * 16, 16), 16)
            mean, dev = spans[0, some, :], spans[1, some, :]
            for part in range(quarter // 128):
                packed = words[dg, m, some, part * 128:(part + 1) * 128]
                for k in range(CODES):
                    code = jnp.right_shift(packed, 2 * k) & 3
                    z = (code.astype(jnp.float32) - mean) * dev
                    z = jnp.where(code == 3, 0.0, z).astype(jnp.bfloat16)
                    at = k * quarter + part * 128
                    scores[slot, there, at:at + 128] = z
            return 0

        lax.fori_loop(0, rows // 16, step, 0, unroll=2)

    decode(0, q, q // 2, (q % 2) * rows)
    for mate in mates:
        wait_recv(words.at[0, mate], w0r.at[mate])

        @pl.when(has_one)
        def _():
            down_one(mate, words.at[0, mate]).start()

        @pl.when(up_two & (mate >= 2))
        def _():
            up_words(mate, words.at[0, mate]).start()

        wait_recv(stats.at[0, mate], s0r.at[mate])
        decode(0, mate, mate // 2, (mate % 2) * rows)

    twin, across = mates[0], mates[1]
    twin_across = lax.rem(twin + 2, GROUP)

    def to_twin(t):
        return remote(parts.at[t, twin], gathered.at[t, 0], ps.at[t, 0], pr.at[t, 0], base + twin)

    def via_twin(t):
        return remote(parts.at[t, twin_across], gathered.at[t, 1], ps.at[t, 1], pr.at[t, 1], base + twin)

    def to_across(t):
        return remote(sums.at[t], gathered.at[t, 2], ps.at[t, 2], pr.at[t, 2], base + across)

    def forward(n):
        t = slots[n]
        wait_recv(gathered.at[t, 1], pr.at[t, 1])
        sums[t] = (accs[t, across] + gathered[t, 1].astype(jnp.float32)).astype(jnp.bfloat16)
        to_across(t).start()

    def product(t, slot, halves):
        right = scores[slot]
        for half in range(halves):
            block = lax.dot_general(
                scores[half], right, (((1,), (1,)), ((), ())), preferred_element_type=jnp.float32
            )
            accs[t, 2 * half] = block[:rows]
            accs[t, 2 * half + 1] = block[rows:]
            parts[t, 2 * half] = block[:rows].astype(jnp.bfloat16)
            parts[t, 2 * half + 1] = block[rows:].astype(jnp.bfloat16)

    first_pair = q // 2
    steps = [(0, first_pair), (0, 1 - first_pair), (1, first_pair), (1, 1 - first_pair), (2, 0)]
    slots = [first_pair, 1 - first_pair, 2 + first_pair, 3 - first_pair, 4]

    own_pos = jnp.concatenate([stats[0, q]] * (rows // 8), axis=0).T
    own_at = own_pos[:, 4:5].astype(jnp.int32) * SPLIT + own_pos[:, 6:7].astype(jnp.int32)

    def reach_of(n, m2):
        dg, pair = steps[n]
        return (m2 + 2 - 2 * GROUP if dg == 2 else dg * GROUP + 2 * pair + m2) - q

    def mirror_copy(t, m2, offset):
        slot = jnp.where(offset > 0, offset - 1, REACH - 1 - offset)
        return remote(mirror.at[t, m2], came.at[slot], ms.at[t, m2], mr.at[slot], me + offset)

    def finish(n):
        dg, pair = steps[n]
        t = slots[n]
        total = accs[t, q]
        for source in (0, 2):
            wait_recv(gathered.at[t, source], pr.at[t, source])
            total = total + gathered[t, source].astype(jnp.float32)
        total = total / samples
        for m2 in range(2):
            m = 2 * pair + m2
            offset = reach_of(n, m2)
            st = stats[dg, m]
            their = st[4:5, :].astype(jnp.int32) * SPLIT + st[6:7, :].astype(jnp.int32)
            block = total[:, m2 * rows:(m2 + 1) * rows]
            block = jnp.where(jnp.abs(own_at - their) <= BAND_BP, block, 0.0)
            cols = pl.ds(pl.multiple_of((REACH + offset) * rows, rows), rows)
            if dg == 0:
                out[:, cols] = block
            else:
                @pl.when((offset <= REACH) & (offset >= -REACH))
                def _():
                    out[:, cols] = block
                    mirror[t, m2] = block.astype(jnp.bfloat16)
                    mirror_copy(t, m2, offset).start()

    def run(n):
        dg, pair = steps[n]
        if dg == 0:
            slot = pair
        else:
            slot = n
            for m2 in range(2):
                m = 2 * pair + m2
                wait_recv(words.at[dg, m], (w1r if dg == 1 else w2r).at[m])
                wait_recv(stats.at[dg, m], (s1r if dg == 1 else s2r).at[m])
                decode(dg, m, slot, m2 * rows)
        product(slots[n], slot, 1 if dg == 2 else 2)
        if dg == 2:
            @pl.when(q < 2)
            def _():
                to_twin(slots[n]).start()

            @pl.when(q >= 2)
            def _():
                via_twin(slots[n]).start()
        else:
            via_twin(slots[n]).start()
            to_twin(slots[n]).start()

    run(0)
    run(1)
    forward(0)

    @pl.when(has_two)
    def _():
        run(4)

    forward(1)

    @pl.when(up_one)
    def _():
        run(2)

    @pl.when(has_two & (q >= 2))
    def _():
        forward(4)

    finish(0)
    finish(1)

    @pl.when(up_one)
    def _():
        forward(2)
        run(3)
        forward(3)

    @pl.when(has_two & (q < 2))
    def _():
        finish(4)

    @pl.when(up_one)
    def _():
        finish(2)
        finish(3)

    def take(slot, col):
        wait_recv(came.at[slot], mr.at[slot])
        out[:, col * rows:(col + 1) * rows] = came[slot].astype(jnp.float32).T

    for offset in range(1, REACH + 1):
        if offset > GROUP:
            @pl.when((offset + q >= 2 * GROUP) & up_two)
            def _():
                take(REACH + offset - 1, REACH + offset)

        @pl.when((offset > q) & (offset <= q + GROUP) & has_one)
        def _():
            take(offset - 1, REACH - offset)

    for i in range(3):
        word_copy(i).wait_send()
        stat_mate(i).wait_send()

    @pl.when(has_one)
    def _():
        for m in range(GROUP):
            stat_one(m).wait_send()
            down_one(m, words.at[0, m]).wait_send()

    @pl.when(up_two)
    def _():
        for m in (2, 3):
            up_words(m, words.at[0, m]).wait_send()

    @pl.when(up_two & (q >= 2))
    def _():
        for m in range(GROUP):
            stat_two(m).wait_send()

    def left(n):
        for copy in (to_twin, via_twin, to_across):
            copy(slots[n]).wait_send()

    left(0)
    left(1)

    @pl.when(up_one)
    def _():
        left(2)
        left(3)

    @pl.when(has_two & (q < 2))
    def _():
        to_twin(4).wait_send()

    @pl.when(has_two & (q >= 2))
    def _():
        via_twin(4).wait_send()
        to_across(4).wait_send()

    for n, there in ((2, up_one), (3, up_one), (4, has_two & (q < 2))):
        for m2 in range(2):
            offset = reach_of(n, m2)

            @pl.when(there & (offset <= REACH) & (offset >= -REACH))
            def _():
                mirror_copy(slots[n], m2, offset).wait_send()


def per_device(devices, genotypes, positions):
    rows, width = genotypes.shape
    quarter = width // GROUP
    dma = pltpu.SemaphoreType.DMA
    vmem = pl.BlockSpec(memory_space=pltpu.VMEM)
    return pl.pallas_call(
        functools.partial(kernel, devices),
        out_shape=jax.ShapeDtypeStruct((rows, (2 * REACH + 1) * rows), jnp.float32),
        in_specs=[vmem, vmem],
        out_specs=vmem,
        scratch_shapes=[
            pltpu.VMEM((3, GROUP, rows, quarter), jnp.int32),
            pltpu.VMEM((3, GROUP, 8, rows), jnp.float32),
            pltpu.VMEM((5, 2 * rows, CODES * quarter), jnp.bfloat16),
            pltpu.VMEM((5, GROUP, rows, 2 * rows), jnp.float32),
            pltpu.VMEM((5, GROUP, rows, 2 * rows), jnp.bfloat16),
            pltpu.VMEM((5, 3, rows, 2 * rows), jnp.bfloat16),
            pltpu.VMEM((5, rows, 2 * rows), jnp.bfloat16),
            pltpu.VMEM((5, 2, rows, rows), jnp.bfloat16),
            pltpu.VMEM((2 * REACH, rows, rows), jnp.bfloat16),
            pltpu.VMEM((2, rows, 128), jnp.float32),
            dma((3,)), dma((GROUP,)),
            dma((GROUP,)), dma((GROUP,)),
            dma((GROUP,)), dma((GROUP,)),
            dma((3,)), dma((GROUP,)),
            dma((GROUP,)), dma((GROUP,)),
            dma((GROUP,)), dma((GROUP,)),
            dma((5, 3)), dma((5, 3)),
            dma((5, 2)), dma((2 * REACH,)),
        ],
        compiler_params=pltpu.CompilerParams(
            collective_id=0, has_side_effects=True, vmem_limit_bytes=60000000
        ),
    )(genotypes, positions[None, :])


def solution(mesh):
    return jax.shard_map(
        functools.partial(per_device, mesh.shape["snp"]),
        mesh=mesh,
        in_specs=(P(("arm", "snp"), None), P(("arm", "snp"))),
        out_specs=P(("arm", "snp"), None),
        check_vma=False,
    )
```

```python
import functools

import jax
import jax.numpy as jnp
from jax import lax
from jax.experimental import pallas as pl
from jax.experimental.pallas import tpu as pltpu
from jax.sharding import PartitionSpec as P

REACH = 6
BAND_BP = 1000000
CODES = 16
GROUP = 4
SPLIT = 4096
MESH = pl.DeviceIdType.MESH


def kernel(
    devices, geno, pos, out, words, stats, scores, accs, parts, gathered, sums, mirror, came, spans,
    w0s, w0r, w1s, w1r, w2s, w2r, s0s, s0r, s1s, s1r, s2s, s2r, ps, pr, ms, mr,
):
    rows, width = geno.shape
    quarter = width // GROUP
    groups = devices // GROUP
    samples = CODES * width
    me = lax.axis_index("snp")
    g, q = me // GROUP, me % GROUP
    base = me - q
    mates = [q + 1 - 2 * lax.rem(q, 2), lax.rem(q + 2, GROUP), None]
    mates[2] = mates[1] + 1 - 2 * lax.rem(mates[1], 2)

    def remote(src, dst, ss, rs, target):
        return pltpu.make_async_remote_copy(
            src_ref=src, dst_ref=dst, send_sem=ss, recv_sem=rs,
            device_id={"snp": target}, device_id_type=MESH,
        )

    barrier = pltpu.get_barrier_semaphore()
    for mate in mates:
        pl.semaphore_signal(barrier, inc=1, device_id={"snp": base + mate}, device_id_type=MESH)
    for dg in (-2, -1, 1, 2):
        @pl.when((g + dg >= 0) & (g + dg < groups))
        def _():
            for m in range(GROUP):
                pl.semaphore_signal(
                    barrier, inc=1, device_id={"snp": base + dg * GROUP + m}, device_id_type=MESH
                )

    low = 0x55555555
    raw = geno[...]
    up = jnp.right_shift(raw, 1)
    miss = raw & up & low
    ones = raw & low & ~miss
    twos = up & low & ~miss

    def count(x):
        x = (x & 0x33333333) + (jnp.right_shift(x, 2) & 0x33333333)
        x = (x & 0x0F0F0F0F) + (jnp.right_shift(x, 4) & 0x0F0F0F0F)
        x = x + jnp.right_shift(x, 8)
        x = (x + jnp.right_shift(x, 16)) & 0x3F
        return jnp.sum(x.astype(jnp.float32), axis=1, keepdims=True)

    tally = samples - count(miss)
    allele = (count(ones) + 2.0 * count(twos) + 1.0) / (2.0 * tally + 2.0)
    spread = lax.rsqrt(2.0 * allele * (1.0 - allele))
    lane = lax.broadcasted_iota(jnp.int32, (rows, 128), 1)
    pair_t = jnp.where(lane < 2, 2.0 * allele, spread).T
    where_row = pos[...]
    hi = where_row // SPLIT
    lo = where_row - hi * SPLIT
    stats[0, q, 0:4, :] = pair_t[0:4, :]
    stats[0, q, 4:6, :] = jnp.broadcast_to(hi.astype(jnp.float32), (2, rows))
    stats[0, q, 6:8, :] = jnp.broadcast_to(lo.astype(jnp.float32), (2, rows))
    own_cols = pl.ds(pl.multiple_of(q * quarter, quarter), quarter)
    words[0, q] = geno[:, own_cols]
    out[...] = jnp.zeros_like(out)

    near = jnp.minimum(g, 2) + jnp.minimum(groups - 1 - g, 2)
    pl.semaphore_wait(barrier, 3 + GROUP * near)

    def word_copy(i):
        mate = mates[i]
        cols = pl.ds(pl.multiple_of(mate * quarter, quarter), quarter)
        return remote(geno.at[:, cols], words.at[0, q], w0s.at[i], w0r.at[q], base + mate)

    def down_one(m, src):
        return remote(src, words.at[1, m], w1s.at[m], w1r.at[m], me - GROUP)

    def up_words(m, src):
        return remote(src, words.at[2, m - 2], w2s.at[m - 2], w2r.at[m - 2], me + 2 * GROUP)

    def stat_mate(i):
        return remote(stats.at[0, q], stats.at[0, q], s0s.at[i], s0r.at[q], base + mates[i])

    def stat_one(m):
        return remote(stats.at[0, q], stats.at[1, q], s1s.at[m], s1r.at[q], base - GROUP + m)

    def stat_two(m):
        return remote(stats.at[0, q], stats.at[2, q - 2], s2s.at[m], s2r.at[q - 2], base + 2 * GROUP + m)

    has_one, has_two = g >= 1, g >= 2
    up_one, up_two = g + 1 < groups, g + 2 < groups

    for i in range(3):
        stat_mate(i).start()
        word_copy(i).start()

    @pl.when(has_one)
    def _():
        down_one(q, geno.at[:, own_cols]).start()
        for m in range(GROUP):
            stat_one(m).start()

    @pl.when(up_two & (q >= 2))
    def _():
        up_words(q, geno.at[:, own_cols]).start()
        for m in range(GROUP):
            stat_two(m).start()

    def wait_recv(ref, sem):
        remote(ref, ref, sem, sem, me).wait_recv()

    def decode(dg, m, slot, row0):
        st = jnp.concatenate([stats[dg, m]] * (rows // 8), axis=0).T
        spans[0] = jnp.broadcast_to(st[:, 0:1], (rows, 128))
        spans[1] = jnp.broadcast_to(st[:, 2:3], (rows, 128))

        def step(r, _):
            some = pl.ds(pl.multiple_of(r * 16, 16), 16)
            there = pl.ds(pl.multiple_of(row0 + r * 16, 16), 16)
            mean, dev = spans[0, some, :], spans[1, some, :]
            for part in range(quarter // 128):
                packed = words[dg, m, some, part * 128:(part + 1) * 128]
                for k in range(CODES):
                    code = jnp.right_shift(packed, 2 * k) & 3
                    z = (code.astype(jnp.float32) - mean) * dev
                    z = jnp.where(code == 3, 0.0, z).astype(jnp.bfloat16)
                    at = k * quarter + part * 128
                    scores[slot, there, at:at + 128] = z
            return 0

        lax.fori_loop(0, rows // 16, step, 0, unroll=2)

    decode(0, q, q // 2, (q % 2) * rows)
    for mate in mates:
        wait_recv(words.at[0, mate], w0r.at[mate])

        @pl.when(has_one)
        def _():
            down_one(mate, words.at[0, mate]).start()

        @pl.when(up_two & (mate >= 2))
        def _():
            up_words(mate, words.at[0, mate]).start()

        wait_recv(stats.at[0, mate], s0r.at[mate])
        decode(0, mate, mate // 2, (mate % 2) * rows)

    twin, across = mates[0], mates[1]
    twin_across = lax.rem(twin + 2, GROUP)

    def to_twin(t):
        return remote(parts.at[t, twin], gathered.at[t, 0], ps.at[t, 0], pr.at[t, 0], base + twin)

    def via_twin(t):
        return remote(parts.at[t, twin_across], gathered.at[t, 1], ps.at[t, 1], pr.at[t, 1], base + twin)

    def to_across(t):
        return remote(sums.at[t], gathered.at[t, 2], ps.at[t, 2], pr.at[t, 2], base + across)

    def forward(n):
        t = slots[n]
        wait_recv(gathered.at[t, 1], pr.at[t, 1])
        sums[t] = (accs[t, across] + gathered[t, 1].astype(jnp.float32)).astype(jnp.bfloat16)
        to_across(t).start()

    def product(t, slot, halves):
        right = scores[slot]
        for half in range(halves):
            block = lax.dot_general(
                scores[half], right, (((1,), (1,)), ((), ())), preferred_element_type=jnp.float32
            )
            accs[t, 2 * half] = block[:rows]
            accs[t, 2 * half + 1] = block[rows:]
            parts[t, 2 * half] = block[:rows].astype(jnp.bfloat16)
            parts[t, 2 * half + 1] = block[rows:].astype(jnp.bfloat16)

    first_pair = q // 2
    steps = [(0, first_pair), (0, 1 - first_pair), (1, first_pair), (1, 1 - first_pair), (2, 0)]
    slots = [first_pair, 1 - first_pair, 2 + first_pair, 3 - first_pair, 4]

    own_pos = jnp.concatenate([stats[0, q]] * (rows // 8), axis=0).T
    own_at = own_pos[:, 4:5].astype(jnp.int32) * SPLIT + own_pos[:, 6:7].astype(jnp.int32)

    def reach_of(n, m2):
        dg, pair = steps[n]
        return (m2 + 2 - 2 * GROUP if dg == 2 else dg * GROUP + 2 * pair + m2) - q

    def mirror_copy(t, m2, offset):
        slot = jnp.where(offset > 0, offset - 1, REACH - 1 - offset)
        return remote(mirror.at[t, m2], came.at[slot], ms.at[t, m2], mr.at[slot], me + offset)

    def finish(n):
        dg, pair = steps[n]
        t = slots[n]
        total = accs[t, q]
        for source in (0, 2):
            wait_recv(gathered.at[t, source], pr.at[t, source])
            total = total + gathered[t, source].astype(jnp.float32)
        total = total / samples
        for m2 in range(2):
            m = 2 * pair + m2
            offset = reach_of(n, m2)
            st = stats[dg, m]
            their = st[4:5, :].astype(jnp.int32) * SPLIT + st[6:7, :].astype(jnp.int32)
            block = total[:, m2 * rows:(m2 + 1) * rows]
            block = jnp.where(jnp.abs(own_at - their) <= BAND_BP, block, 0.0)
            cols = pl.ds(pl.multiple_of((REACH + offset) * rows, rows), rows)
            if dg == 0:
                out[:, cols] = block
            else:
                @pl.when((offset <= REACH) & (offset >= -REACH))
                def _():
                    out[:, cols] = block
                    mirror[t, m2] = block.astype(jnp.bfloat16)
                    mirror_copy(t, m2, offset).start()

    def ready(n):
        dg, pair = steps[n]
        for m2 in range(2):
            m = 2 * pair + m2
            wait_recv(words.at[dg, m], (w1r if dg == 1 else w2r).at[m])
            wait_recv(stats.at[dg, m], (s1r if dg == 1 else s2r).at[m])
            decode(dg, m, n, m2 * rows)

    def combine(n):
        dg, pair = steps[n]
        product(slots[n], pair if dg == 0 else n, 1 if dg == 2 else 2)
        if dg == 2:
            @pl.when(q < 2)
            def _():
                to_twin(slots[n]).start()

            @pl.when(q >= 2)
            def _():
                via_twin(slots[n]).start()
        else:
            via_twin(slots[n]).start()
            to_twin(slots[n]).start()

    combine(0)

    @pl.when(has_two)
    def _():
        ready(4)
        combine(4)

    forward(0)

    @pl.when(up_one)
    def _():
        ready(2)
        combine(2)

    @pl.when(has_two & (q >= 2))
    def _():
        forward(4)

    @pl.when(up_one)
    def _():
        ready(3)
        forward(2)
        combine(3)

    @pl.when(has_two & (q < 2))
    def _():
        finish(4)

    combine(1)

    @pl.when(up_one)
    def _():
        forward(3)

    forward(1)

    @pl.when(up_one)
    def _():
        finish(2)
        finish(3)

    finish(0)
    finish(1)

    def take(slot, col):
        wait_recv(came.at[slot], mr.at[slot])
        out[:, col * rows:(col + 1) * rows] = came[slot].astype(jnp.float32).T

    for offset in range(1, REACH + 1):
        if offset > GROUP:
            @pl.when((offset + q >= 2 * GROUP) & up_two)
            def _():
                take(REACH + offset - 1, REACH + offset)

        @pl.when((offset > q) & (offset <= q + GROUP) & has_one)
        def _():
            take(offset - 1, REACH - offset)

    for i in range(3):
        word_copy(i).wait_send()
        stat_mate(i).wait_send()

    @pl.when(has_one)
    def _():
        for m in range(GROUP):
            stat_one(m).wait_send()
            down_one(m, words.at[0, m]).wait_send()

    @pl.when(up_two)
    def _():
        for m in (2, 3):
            up_words(m, words.at[0, m]).wait_send()

    @pl.when(up_two & (q >= 2))
    def _():
        for m in range(GROUP):
            stat_two(m).wait_send()

    def left(n):
        for copy in (to_twin, via_twin, to_across):
            copy(slots[n]).wait_send()

    left(0)
    left(1)

    @pl.when(up_one)
    def _():
        left(2)
        left(3)

    @pl.when(has_two & (q < 2))
    def _():
        to_twin(4).wait_send()

    @pl.when(has_two & (q >= 2))
    def _():
        via_twin(4).wait_send()
        to_across(4).wait_send()

    for n, there in ((2, up_one), (3, up_one), (4, has_two & (q < 2))):
        for m2 in range(2):
            offset = reach_of(n, m2)

            @pl.when(there & (offset <= REACH) & (offset >= -REACH))
            def _():
                mirror_copy(slots[n], m2, offset).wait_send()


def per_device(devices, genotypes, positions):
    rows, width = genotypes.shape
    quarter = width // GROUP
    dma = pltpu.SemaphoreType.DMA
    vmem = pl.BlockSpec(memory_space=pltpu.VMEM)
    return pl.pallas_call(
        functools.partial(kernel, devices),
        out_shape=jax.ShapeDtypeStruct((rows, (2 * REACH + 1) * rows), jnp.float32),
        in_specs=[vmem, vmem],
        out_specs=vmem,
        scratch_shapes=[
            pltpu.VMEM((3, GROUP, rows, quarter), jnp.int32),
            pltpu.VMEM((3, GROUP, 8, rows), jnp.float32),
            pltpu.VMEM((5, 2 * rows, CODES * quarter), jnp.bfloat16),
            pltpu.VMEM((5, GROUP, rows, 2 * rows), jnp.float32),
            pltpu.VMEM((5, GROUP, rows, 2 * rows), jnp.bfloat16),
            pltpu.VMEM((5, 3, rows, 2 * rows), jnp.bfloat16),
            pltpu.VMEM((5, rows, 2 * rows), jnp.bfloat16),
            pltpu.VMEM((5, 2, rows, rows), jnp.bfloat16),
            pltpu.VMEM((2 * REACH, rows, rows), jnp.bfloat16),
            pltpu.VMEM((2, rows, 128), jnp.float32),
            dma((3,)), dma((GROUP,)),
            dma((GROUP,)), dma((GROUP,)),
            dma((GROUP,)), dma((GROUP,)),
            dma((3,)), dma((GROUP,)),
            dma((GROUP,)), dma((GROUP,)),
            dma((GROUP,)), dma((GROUP,)),
            dma((5, 3)), dma((5, 3)),
            dma((5, 2)), dma((2 * REACH,)),
        ],
        compiler_params=pltpu.CompilerParams(
            collective_id=0, has_side_effects=True, vmem_limit_bytes=60000000
        ),
    )(genotypes, positions[None, :])


def solution(mesh):
    return jax.shard_map(
        functools.partial(per_device, mesh.shape["snp"]),
        mesh=mesh,
        in_specs=(P(("arm", "snp"), None), P(("arm", "snp"))),
        out_specs=P(("arm", "snp"), None),
        check_vma=False,
    )
```

```python
import functools

import jax
import jax.numpy as jnp
from jax import lax
from jax.experimental import pallas as pl
from jax.experimental.pallas import tpu as pltpu
from jax.sharding import PartitionSpec as P

REACH = 6
BAND_BP = 1000000
CODES = 16
GROUP = 4
SPLIT = 4096
MESH = pl.DeviceIdType.MESH


def kernel(
    devices, geno, pos, out, words, stats, scores, accs, parts, gathered, sums, mirror, came, spans,
    w0s, w0r, w1s, w1r, w2s, w2r, s0s, s0r, s1s, s1r, s2s, s2r, ps, pr, ms, mr,
):
    rows, width = geno.shape
    quarter = width // GROUP
    groups = devices // GROUP
    samples = CODES * width
    me = lax.axis_index("snp")
    g, q = me // GROUP, me % GROUP
    base = me - q
    mates = [q + 1 - 2 * lax.rem(q, 2), lax.rem(q + 2, GROUP), None]
    mates[2] = mates[1] + 1 - 2 * lax.rem(mates[1], 2)

    def remote(src, dst, ss, rs, target):
        return pltpu.make_async_remote_copy(
            src_ref=src, dst_ref=dst, send_sem=ss, recv_sem=rs,
            device_id={"snp": target}, device_id_type=MESH,
        )

    barrier = pltpu.get_barrier_semaphore()
    for mate in mates:
        pl.semaphore_signal(barrier, inc=1, device_id={"snp": base + mate}, device_id_type=MESH)
    for dg in (-2, -1, 1, 2):
        @pl.when((g + dg >= 0) & (g + dg < groups))
        def _():
            for m in range(GROUP):
                pl.semaphore_signal(
                    barrier, inc=1, device_id={"snp": base + dg * GROUP + m}, device_id_type=MESH
                )

    low = 0x55555555
    raw = geno[...]
    up = jnp.right_shift(raw, 1)
    miss = raw & up & low
    ones = raw & low & ~miss
    twos = up & low & ~miss

    def count(x):
        x = (x & 0x33333333) + (jnp.right_shift(x, 2) & 0x33333333)
        x = (x & 0x0F0F0F0F) + (jnp.right_shift(x, 4) & 0x0F0F0F0F)
        x = x + jnp.right_shift(x, 8)
        x = (x + jnp.right_shift(x, 16)) & 0x3F
        return jnp.sum(x.astype(jnp.float32), axis=1, keepdims=True)

    tally = samples - count(miss)
    allele = (count(ones) + 2.0 * count(twos) + 1.0) / (2.0 * tally + 2.0)
    spread = lax.rsqrt(2.0 * allele * (1.0 - allele))
    lane = lax.broadcasted_iota(jnp.int32, (rows, 128), 1)
    pair_t = jnp.where(lane < 2, 2.0 * allele, spread).T
    where_row = pos[...]
    hi = where_row // SPLIT
    lo = where_row - hi * SPLIT
    stats[0, q, 0:4, :] = pair_t[0:4, :]
    stats[0, q, 4:6, :] = jnp.broadcast_to(hi.astype(jnp.float32), (2, rows))
    stats[0, q, 6:8, :] = jnp.broadcast_to(lo.astype(jnp.float32), (2, rows))
    own_cols = pl.ds(pl.multiple_of(q * quarter, quarter), quarter)
    words[0, q] = geno[:, own_cols]
    out[...] = jnp.zeros_like(out)

    near = jnp.minimum(g, 2) + jnp.minimum(groups - 1 - g, 2)
    pl.semaphore_wait(barrier, 3 + GROUP * near)

    def word_copy(i):
        mate = mates[i]
        cols = pl.ds(pl.multiple_of(mate * quarter, quarter), quarter)
        return remote(geno.at[:, cols], words.at[0, q], w0s.at[i], w0r.at[q], base + mate)

    def down_one(m, src):
        return remote(src, words.at[1, m], w1s.at[m], w1r.at[m], me - GROUP)

    def up_words(m, src):
        return remote(src, words.at[2, m - 2], w2s.at[m - 2], w2r.at[m - 2], me + 2 * GROUP)

    def stat_mate(i):
        return remote(stats.at[0, q], stats.at[0, q], s0s.at[i], s0r.at[q], base + mates[i])

    def stat_one(m):
        return remote(stats.at[0, q], stats.at[1, q], s1s.at[m], s1r.at[q], base - GROUP + m)

    def stat_two(m):
        return remote(stats.at[0, q], stats.at[2, q - 2], s2s.at[m], s2r.at[q - 2], base + 2 * GROUP + m)

    has_one, has_two = g >= 1, g >= 2
    up_one, up_two = g + 1 < groups, g + 2 < groups

    for i in range(3):
        stat_mate(i).start()
        word_copy(i).start()

    @pl.when(has_one)
    def _():
        down_one(q, geno.at[:, own_cols]).start()
        for m in range(GROUP):
            stat_one(m).start()

    @pl.when(up_two & (q >= 2))
    def _():
        up_words(q, geno.at[:, own_cols]).start()
        for m in range(GROUP):
            stat_two(m).start()

    def wait_recv(ref, sem):
        remote(ref, ref, sem, sem, me).wait_recv()

    def decode(dg, m, slot, row0):
        st = jnp.concatenate([stats[dg, m]] * (rows // 8), axis=0).T
        spans[0] = jnp.broadcast_to(st[:, 0:1], (rows, 128))
        spans[1] = jnp.broadcast_to(st[:, 2:3], (rows, 128))

        def step(r, _):
            some = pl.ds(pl.multiple_of(r * 16, 16), 16)
            there = pl.ds(pl.multiple_of(row0 + r * 16, 16), 16)
            mean, dev = spans[0, some, :], spans[1, some, :]
            for part in range(quarter // 128):
                packed = words[dg, m, some, part * 128:(part + 1) * 128]
                for k in range(CODES):
                    code = jnp.right_shift(packed, 2 * k) & 3
                    z = (code.astype(jnp.float32) - mean) * dev
                    z = jnp.where(code == 3, 0.0, z).astype(jnp.bfloat16)
                    at = k * quarter + part * 128
                    scores[slot, there, at:at + 128] = z
            return 0

        lax.fori_loop(0, rows // 16, step, 0, unroll=2)

    decode(0, q, q // 2, (q % 2) * rows)
    for mate in mates:
        wait_recv(words.at[0, mate], w0r.at[mate])

        @pl.when(has_one)
        def _():
            down_one(mate, words.at[0, mate]).start()

        @pl.when(up_two & (mate >= 2))
        def _():
            up_words(mate, words.at[0, mate]).start()

        wait_recv(stats.at[0, mate], s0r.at[mate])
        decode(0, mate, mate // 2, (mate % 2) * rows)

    twin, across = mates[0], mates[1]
    twin_across = lax.rem(twin + 2, GROUP)

    def to_twin(t):
        return remote(parts.at[t, twin], gathered.at[t, 0], ps.at[t, 0], pr.at[t, 0], base + twin)

    def via_twin(t):
        return remote(parts.at[t, twin_across], gathered.at[t, 1], ps.at[t, 1], pr.at[t, 1], base + twin)

    def to_across(t):
        return remote(sums.at[t], gathered.at[t, 2], ps.at[t, 2], pr.at[t, 2], base + across)

    def forward(n):
        t = slots[n]
        wait_recv(gathered.at[t, 1], pr.at[t, 1])
        sums[t] = (accs[t, across] + gathered[t, 1].astype(jnp.float32)).astype(jnp.bfloat16)
        to_across(t).start()

    def product(t, slot, halves):
        right = scores[slot]
        for half in range(halves):
            block = lax.dot_general(
                scores[half], right, (((1,), (1,)), ((), ())), preferred_element_type=jnp.float32
            )
            accs[t, 2 * half] = block[:rows]
            accs[t, 2 * half + 1] = block[rows:]
            parts[t, 2 * half] = block[:rows].astype(jnp.bfloat16)
            parts[t, 2 * half + 1] = block[rows:].astype(jnp.bfloat16)

    first_pair = 0
    steps = [(0, first_pair), (0, 1 - first_pair), (1, first_pair), (1, 1 - first_pair), (2, 0)]
    slots = [first_pair, 1 - first_pair, 2 + first_pair, 3 - first_pair, 4]

    own_pos = jnp.concatenate([stats[0, q]] * (rows // 8), axis=0).T
    own_at = own_pos[:, 4:5].astype(jnp.int32) * SPLIT + own_pos[:, 6:7].astype(jnp.int32)

    def reach_of(n, m2):
        dg, pair = steps[n]
        return (m2 + 2 - 2 * GROUP if dg == 2 else dg * GROUP + 2 * pair + m2) - q

    def mirror_copy(t, m2, offset):
        slot = jnp.where(offset > 0, offset - 1, REACH - 1 - offset)
        return remote(mirror.at[t, m2], came.at[slot], ms.at[t, m2], mr.at[slot], me + offset)

    def finish(n):
        dg, pair = steps[n]
        t = slots[n]
        total = accs[t, q]
        for source in (0, 2):
            wait_recv(gathered.at[t, source], pr.at[t, source])
            total = total + gathered[t, source].astype(jnp.float32)
        total = total / samples
        for m2 in range(2):
            m = 2 * pair + m2
            offset = reach_of(n, m2)
            st = stats[dg, m]
            their = st[4:5, :].astype(jnp.int32) * SPLIT + st[6:7, :].astype(jnp.int32)
            block = total[:, m2 * rows:(m2 + 1) * rows]
            block = jnp.where(jnp.abs(own_at - their) <= BAND_BP, block, 0.0)
            cols = pl.ds(pl.multiple_of((REACH + offset) * rows, rows), rows)
            if dg == 0:
                out[:, cols] = block
            else:
                @pl.when((offset <= REACH) & (offset >= -REACH))
                def _():
                    out[:, cols] = block
                    mirror[t, m2] = block.astype(jnp.bfloat16)
                    mirror_copy(t, m2, offset).start()

    def ready(n):
        dg, pair = steps[n]
        for m2 in range(2):
            m = 2 * pair + m2
            wait_recv(words.at[dg, m], (w1r if dg == 1 else w2r).at[m])
            wait_recv(stats.at[dg, m], (s1r if dg == 1 else s2r).at[m])
            decode(dg, m, n, m2 * rows)

    def combine(n):
        dg, pair = steps[n]
        product(slots[n], pair if dg == 0 else n, 1 if dg == 2 else 2)
        if dg == 2:
            @pl.when(q < 2)
            def _():
                to_twin(slots[n]).start()

            @pl.when(q >= 2)
            def _():
                via_twin(slots[n]).start()
        else:
            via_twin(slots[n]).start()
            to_twin(slots[n]).start()

    combine(0)

    @pl.when(has_two)
    def _():
        ready(4)
        combine(4)

    forward(0)

    @pl.when(up_one)
    def _():
        ready(2)
        combine(2)

    @pl.when(has_two & (q >= 2))
    def _():
        forward(4)

    @pl.when(up_one)
    def _():
        ready(3)
        forward(2)
        combine(3)

    @pl.when(has_two & (q < 2))
    def _():
        finish(4)

    combine(1)

    @pl.when(up_one)
    def _():
        forward(3)

    @pl.when(up_one)
    def _():
        finish(2)

    forward(1)

    @pl.when(up_one)
    def _():
        finish(3)

    finish(0)
    finish(1)

    def take(slot, col):
        wait_recv(came.at[slot], mr.at[slot])
        out[:, col * rows:(col + 1) * rows] = came[slot].astype(jnp.float32).T

    for offset in range(1, REACH + 1):
        if offset > GROUP:
            @pl.when((offset + q >= 2 * GROUP) & up_two)
            def _():
                take(REACH + offset - 1, REACH + offset)

        @pl.when((offset > q) & (offset <= q + GROUP) & has_one)
        def _():
            take(offset - 1, REACH - offset)

    for i in range(3):
        word_copy(i).wait_send()
        stat_mate(i).wait_send()

    @pl.when(has_one)
    def _():
        for m in range(GROUP):
            stat_one(m).wait_send()
            down_one(m, words.at[0, m]).wait_send()

    @pl.when(up_two)
    def _():
        for m in (2, 3):
            up_words(m, words.at[0, m]).wait_send()

    @pl.when(up_two & (q >= 2))
    def _():
        for m in range(GROUP):
            stat_two(m).wait_send()

    def left(n):
        for copy in (to_twin, via_twin, to_across):
            copy(slots[n]).wait_send()

    left(0)
    left(1)

    @pl.when(up_one)
    def _():
        left(2)
        left(3)

    @pl.when(has_two & (q < 2))
    def _():
        to_twin(4).wait_send()

    @pl.when(has_two & (q >= 2))
    def _():
        via_twin(4).wait_send()
        to_across(4).wait_send()

    for n, there in ((2, up_one), (3, up_one), (4, has_two & (q < 2))):
        for m2 in range(2):
            offset = reach_of(n, m2)

            @pl.when(there & (offset <= REACH) & (offset >= -REACH))
            def _():
                mirror_copy(slots[n], m2, offset).wait_send()


def per_device(devices, genotypes, positions):
    rows, width = genotypes.shape
    quarter = width // GROUP
    dma = pltpu.SemaphoreType.DMA
    vmem = pl.BlockSpec(memory_space=pltpu.VMEM)
    return pl.pallas_call(
        functools.partial(kernel, devices),
        out_shape=jax.ShapeDtypeStruct((rows, (2 * REACH + 1) * rows), jnp.float32),
        in_specs=[vmem, vmem],
        out_specs=vmem,
        scratch_shapes=[
            pltpu.VMEM((3, GROUP, rows, quarter), jnp.int32),
            pltpu.VMEM((3, GROUP, 8, rows), jnp.float32),
            pltpu.VMEM((5, 2 * rows, CODES * quarter), jnp.bfloat16),
            pltpu.VMEM((5, GROUP, rows, 2 * rows), jnp.float32),
            pltpu.VMEM((5, GROUP, rows, 2 * rows), jnp.bfloat16),
            pltpu.VMEM((5, 3, rows, 2 * rows), jnp.bfloat16),
            pltpu.VMEM((5, rows, 2 * rows), jnp.bfloat16),
            pltpu.VMEM((5, 2, rows, rows), jnp.bfloat16),
            pltpu.VMEM((2 * REACH, rows, rows), jnp.bfloat16),
            pltpu.VMEM((2, rows, 128), jnp.float32),
            dma((3,)), dma((GROUP,)),
            dma((GROUP,)), dma((GROUP,)),
            dma((GROUP,)), dma((GROUP,)),
            dma((3,)), dma((GROUP,)),
            dma((GROUP,)), dma((GROUP,)),
            dma((GROUP,)), dma((GROUP,)),
            dma((5, 3)), dma((5, 3)),
            dma((5, 2)), dma((2 * REACH,)),
        ],
        compiler_params=pltpu.CompilerParams(
            collective_id=0, has_side_effects=True, vmem_limit_bytes=60000000
        ),
    )(genotypes, positions[None, :])


def solution(mesh):
    return jax.shard_map(
        functools.partial(per_device, mesh.shape["snp"]),
        mesh=mesh,
        in_specs=(P(("arm", "snp"), None), P(("arm", "snp"))),
        out_specs=P(("arm", "snp"), None),
        check_vma=False,
    )
```
